64 devices in a mesh: data: 4 (over x, y), seq: 16 (over z, core).
Axes of the slice: x: 2, y: 2, z: 8, core: 2. Of those that a mesh axis runs over, the one named last changes fastest.
The devices are a block of a 4x4x8 slice.
Arguments:
- x: bfloat16 [16384, 1024], P(('data', 'seq')), parts along dimension 0
- g1: float32 [1024], replicated
- b1: float32 [1024], replicated
- g2: float32 [1024], replicated
- b2: float32 [1024], replicated
- wqkv: bfloat16 [1024, 3072], replicated
- wo: bfloat16 [16, 64, 1024], replicated
- w1: bfloat16 [1024, 4096], replicated
- w2: bfloat16 [4096, 1024], replicated
Outputs:
- output: bfloat16 [16384, 1024], P(('data', 'seq')), parts along dimension 0
There are 4 independent parts. The reference program is written for one: setup_inputs(seed, part) draws one part's arguments, and reference() takes and returns one part's arrays. A program takes and returns all parts, laid end to end along the dimension named above; an argument that names none is the same for every part.
All inputs are finite; a program needn't handle non-finite values.
Results may differ from the reference program's by a relative error of at most 0.00216896.
Values are sent between devices in bfloat16 or wider.
A program may use at most 768 MiB of HBM per device.

```python
import jax
import jax.numpy as jnp
from jax import lax

S = 4096
D = 1024
H = 16
DH = 64
F = 4096
QB = 128

EPS = 1e-5
SCALE = DH ** -0.5
NEG = -1e30


def setup_inputs(seed: int = 0, part: int = 0) -> dict:
    key = jax.random.PRNGKey(seed)
    k_shared, k_part = jax.random.split(key)
    kp = jax.random.fold_in(k_part, part)
    kx, ku, kf, kph = jax.random.split(kp, 4)
    ks = jax.random.split(k_shared, 8)
    nf = 4
    t = jnp.arange(S, dtype=jnp.float32) / S
    freq = jax.random.uniform(kf, (nf,), jnp.float32, 0.25, 2.0)
    phase = jax.random.uniform(kph, (nf,), jnp.float32, 0.0, 6.2831853)
    waves = jnp.sin(6.2831853 * freq[None, :] * t[:, None] + phase[None, :])
    u = jax.random.normal(ku, (nf, D), jnp.float32)
    smooth = jnp.dot(waves, u) * (2.0 / nf) ** 0.5
    x = 0.6 * jax.random.normal(kx, (S, D), jnp.float32) + smooth

    def w(k, shape, fan_in):
        return (jax.random.normal(k, shape, jnp.float32) * fan_in ** -0.5).astype(jnp.bfloat16)

    return {
        "x": x.astype(jnp.bfloat16),
        "g1": 1.0 + 0.2 * jax.random.normal(ks[0], (D,), jnp.float32),
        "b1": 0.2 * jax.random.normal(ks[1], (D,), jnp.float32),
        "g2": 1.0 + 0.2 * jax.random.normal(ks[2], (D,), jnp.float32),
        "b2": 0.2 * jax.random.normal(ks[3], (D,), jnp.float32),
        "wqkv": w(ks[4], (D, 3 * H * DH), D),
        "wo": w(ks[5], (H, DH, D), H * DH),
        "w1": w(ks[6], (D, F), D),
        "w2": w(ks[7], (F, D), F),
    }


def _layer_norm(x, g, b):
    xf = x.astype(jnp.float32)
    mu = jnp.mean(xf, axis=-1, keepdims=True)
    var = jnp.mean(jnp.square(xf - mu), axis=-1, keepdims=True)
    return ((xf - mu) * lax.rsqrt(var + EPS) * g + b).astype(jnp.bfloat16)


def _rope(t, pos):
    half = DH // 2
    inv = 10000.0 ** (-2.0 * jnp.arange(half, dtype=jnp.float32) / DH)
    ang = pos.astype(jnp.float32)[:, None] * inv[None, :]
    cos = jnp.cos(ang)[:, None, :]
    sin = jnp.sin(ang)[:, None, :]
    tf = t.astype(jnp.float32)
    a, b = tf[..., :half], tf[..., half:]
    return jnp.concatenate([a * cos - b * sin, b * cos + a * sin], axis=-1).astype(jnp.bfloat16)


def _head_attention(qh, kh, vh):
    rows = jnp.arange(S).reshape(S // QB, QB)
    cols = jnp.arange(S)

    def block(args):
        qb, rb = args
        s = jnp.dot(qb, kh.T, preferred_element_type=jnp.float32) * SCALE
        s = jnp.where(cols[None, :] <= rb[:, None], s, NEG)
        p = jax.nn.softmax(s, axis=-1).astype(jnp.bfloat16)
        return jnp.dot(p, vh, preferred_element_type=jnp.float32).astype(jnp.bfloat16)

    return lax.map(block, (qh.reshape(S // QB, QB, DH), rows)).reshape(S, DH)


def reference(x, g1, b1, g2, b2, wqkv, wo, w1, w2):
    pos = jnp.arange(S)
    a = _layer_norm(x, g1, b1)
    qkv = jnp.dot(a, wqkv, preferred_element_type=jnp.float32).astype(jnp.bfloat16).reshape(S, 3, H, DH)
    q = _rope(qkv[:, 0], pos)
    k = _rope(qkv[:, 1], pos)
    v = qkv[:, 2]
    o = lax.map(lambda t: _head_attention(t[0], t[1], t[2]),
                (q.transpose(1, 0, 2), k.transpose(1, 0, 2), v.transpose(1, 0, 2)))
    o = o.transpose(1, 0, 2).reshape(S, H * DH)
    attn = jnp.dot(o, wo.reshape(H * DH, D), preferred_element_type=jnp.float32)
    m = _layer_norm(x, g2, b2)
    h = jax.nn.gelu(jnp.dot(m, w1, preferred_element_type=jnp.float32), approximate=False).astype(jnp.bfloat16)
    mlp = jnp.dot(h, w2, preferred_element_type=jnp.float32)
    return (x.astype(jnp.float32) + attn + mlp).astype(jnp.bfloat16)
```

```python
import functools
import math

import jax
import jax.numpy as jnp
from jax import lax
from jax.experimental import pallas as pl
from jax.experimental.pallas import tpu as pltpu
from jax.sharding import PartitionSpec as P

EPS = 1e-5
NEG = -1e30
F32 = jnp.float32
BF16 = jnp.bfloat16
LANES = 128
HCOL = 512


def _roll(t, shift):
    return pltpu.roll(t, shift, 1)


def _low(shape):
    return lax.broadcasted_iota(jnp.int32, shape, 1) < LANES // 2


def _pair(top, bot):
    low = _low(top.shape)
    return jnp.where(low, top, _roll(bot, LANES // 2)), jnp.where(low, _roll(top, LANES // 2), bot)


def _kernel(n, x_ref, g1_ref, b1_ref, g2_ref, b2_ref, cos_ref, sin_ref, wqkv_ref, wo_ref, w1_ref, w2_ref, y_ref,
            wq_v, wo_v, w1_v, w2_v, a_v, m_v, acc_v, send, recv, s_v, o_send, o_recv, o_v,
            wq_sem, wo_sem, w1_sem, w2_sem, send_sem, recv_sem, osend_sem, orecv_sem):
    r, d = x_ref.shape
    half = r // 2
    chips = n // 2
    ngrp = n // 4
    gcol = d // ngrp
    nm = w1_v.shape[0]
    me = lax.axis_index("seq")
    chip, core = me // 2, me % 2
    g0 = ((chip + chips // 2) % chips) // 2

    barrier = pltpu.get_barrier_semaphore()

    def greet(i, _):
        pl.semaphore_signal(barrier, inc=1, device_id={"seq": (me + i) % n})
        return 0

    lax.fori_loop(1, n, greet, 0)

    def wq_copy(s, t):
        col = pl.multiple_of(t * d + ((g0 + s) % ngrp) * gcol, gcol)
        return pltpu.make_async_copy(wqkv_ref.at[:, pl.ds(col, gcol)], wq_v.at[s, t], wq_sem.at[s, t])

    def w1_copy(i):
        return pltpu.make_async_copy(w1_ref.at[:, pl.ds(pl.multiple_of(i * HCOL, HCOL), HCOL)], w1_v.at[i], w1_sem.at[i])

    def w2_copy(i):
        return pltpu.make_async_copy(w2_ref.at[pl.ds(pl.multiple_of(i * HCOL, HCOL), HCOL), :], w2_v.at[i], w2_sem.at[i])

    wo_copy = pltpu.make_async_copy(wo_ref, wo_v, wo_sem)

    for s in range(ngrp):
        for t in range(3):
            wq_copy(s, t).start()

    xf = x_ref[...].astype(F32)
    mu = jnp.mean(xf, axis=-1, keepdims=True)
    xc = xf - mu
    var = jnp.mean(jnp.square(xc), axis=-1, keepdims=True)
    xn = xc * lax.rsqrt(var + EPS)
    a_v[...] = (xn * g1_ref[...] + b1_ref[...]).astype(BF16)
    m_v[...] = (xn * g2_ref[...] + b2_ref[...]).astype(BF16)
    acc_v[...] = xf
    pl.semaphore_wait(barrier, n - 1)

    def rope(t):
        t = t.astype(BF16).astype(F32)
        lane = lax.broadcasted_iota(jnp.int32, t.shape, 1)
        partner = jnp.where(lane % 64 < 32, _roll(t, LANES - 32), _roll(t, 32))
        return t * cos_ref[...] + partner * sin_ref[...]

    def ship(dst, src, land, ssem, rsem):
        @pl.when(dst == me)
        def _():
            pltpu.make_async_copy(src.at[dst], land.at[me], rsem.at[me]).start()

        @pl.when(dst != me)
        def _():
            pltpu.make_async_remote_copy(
                src_ref=src.at[dst], dst_ref=land.at[me], send_sem=ssem.at[dst], recv_sem=rsem.at[me],
                device_id={"seq": dst}).start()

    def qkv_step(s, _):
        g = (g0 + s) % ngrp
        for t in range(3):
            wq_copy(s, t).wait()
        for i in range(nm // ngrp):
            w1_copy(s * (nm // ngrp) + i).start()
            w2_copy(s * (nm // ngrp) + i).start()
        a = a_v[...]
        q, k, v = (jnp.dot(a, wq_v[s, t], preferred_element_type=F32) for t in range(3))
        for j in range(2):
            cols = slice(j * LANES, (j + 1) * LANES)
            qr, kr, vr = rope(q[:, cols]), rope(k[:, cols]), v[:, cols]
            kv = _pair(kr, vr)
            qq = _pair(qr[:half], qr[half:])
            for e in range(2):
                send[4 * g + 2 * j + e, :r, :] = kv[e].astype(BF16)
                send[4 * g + 2 * j + e, r:, :] = qq[e].astype(BF16)
        for i in range(4):
            ship(4 * g + i, send, recv, send_sem, recv_sem)
        return 0

    lax.fori_loop(0, ngrp, qkv_step, 0)
    wo_copy.start()

    def mlp_step(i, _):
        w1_copy(i).wait()
        w2_copy(i).wait()

        u = jnp.dot(m_v[...], w1_v[i], preferred_element_type=F32)
        h = (0.5 * u * (1.0 + lax.erf(u * (0.5 ** 0.5)))).astype(BF16)
        acc_v[...] += jnp.dot(h, w2_v[i], preferred_element_type=F32)
        return 0

    lax.fori_loop(0, nm, mlp_step, 0)

    def arrived(i, _):
        pltpu.make_async_copy(send.at[i], recv.at[i], recv_sem.at[i]).wait()
        return 0

    lax.fori_loop(0, n, arrived, 0)

    scale = 64.0 ** -0.5 * math.log2(math.e)

    def attend(s, _):
        i = s // 2
        off = chips // 2 + ((i + 1) // 2) * (1 - 2 * (i % 2))
        qi = ((chip + off) % chips) * 2 + (core + 1 + s) % 2
        qp = recv[qi, r:, :].astype(F32)
        low = _low(qp.shape)
        q = jnp.concatenate([jnp.where(low, qp, 0.0), jnp.where(low, _roll(qp, LANES // 2), 0.0)], axis=0).astype(BF16)

        def scores(b):
            return lax.dot_general(q, recv[b, :r, :], (((1,), (1,)), ((), ())), preferred_element_type=F32)

        def top(sc):
            out = sc[:, :LANES]
            for c in range(1, sc.shape[1] // LANES):
                out = jnp.maximum(out, sc[:, c * LANES:(c + 1) * LANES])
            return out

        def first(t, mx):
            for u in range(2):
                sc = scores(2 * t + u)
                s_v[2 * t + u] = sc
                mx = jnp.maximum(mx, top(sc))
            return mx

        nfull = qi // 2
        mx = lax.fori_loop(0, nfull, first, jnp.full((r, LANES), NEG, F32))
        for u in range(2):
            b = 2 * nfull + u
            sc = scores(b)
            rows = qi * r + lax.broadcasted_iota(jnp.int32, sc.shape, 0)
            cols = b * r + lax.broadcasted_iota(jnp.int32, sc.shape, 1)
            sc = jnp.where(cols <= rows, sc, NEG)
            s_v[b] = sc
            mx = jnp.maximum(mx, top(sc))
        mx = jnp.max(mx, axis=1, keepdims=True) * scale

        def second(t, carry):
            den, out = carry
            for u in range(2):
                p = jnp.exp2(s_v[2 * t + u] * scale - mx)
                for c in range(r // LANES):
                    den = den + p[:, c * LANES:(c + 1) * LANES]
                out = out + jnp.dot(p.astype(BF16), recv[2 * t + u, :r, :], preferred_element_type=F32)
            return den, out

        zero = jnp.zeros((r, LANES), F32)
        den, out = lax.fori_loop(0, nfull + 1, second, (zero, zero))
        out = out / jnp.sum(den, axis=1, keepdims=True)
        o_send[qi] = _pair(out[:half], out[half:])[1].astype(BF16)
        ship(qi, o_send, o_recv, osend_sem, orecv_sem)
        return 0

    lax.fori_loop(0, n, attend, 0)

    def returned(i, _):
        pltpu.make_async_copy(o_send.at[i], o_recv.at[i], orecv_sem.at[i]).wait()
        return 0

    lax.fori_loop(0, n, returned, 0)
    for c in range(n // 2):
        p0, p1 = o_recv[2 * c].astype(F32), o_recv[2 * c + 1].astype(F32)
        t, b = _pair(p0, p1)
        o_v[:half, c * LANES:(c + 1) * LANES] = t.astype(BF16)
        o_v[half:, c * LANES:(c + 1) * LANES] = b.astype(BF16)
    wo_copy.wait()
    for c in range(d // 256):
        cols = slice(c * 256, (c + 1) * 256)
        y_ref[:, cols] = (acc_v[:, cols] + jnp.dot(o_v[...], wo_v[:, cols], preferred_element_type=F32)).astype(BF16)

    def drained(i, _):
        @pl.when(i != me)
        def _():
            for buf, land, sem in ((send, recv, send_sem), (o_send, o_recv, osend_sem)):
                pltpu.make_async_copy(buf.at[0], land.at[0], sem.at[i]).wait()
        return 0

    lax.fori_loop(0, n, drained, 0)


def _tables(pos, dh):
    half = dh // 2
    inv = 10000.0 ** (-2.0 * jnp.arange(half, dtype=F32) / dh)
    ang = pos.astype(F32)[:, None] * inv[None, :]
    cos, sin = jnp.cos(ang), jnp.sin(ang)
    return jnp.concatenate([cos] * 4, axis=1), jnp.concatenate([-sin, sin, -sin, sin], axis=1)


def solution(mesh):
    n = mesh.shape["seq"]

    def local(x, g1, b1, g2, b2, wqkv, wo, w1, w2):
        r, d = x.shape
        nh, dh, _ = wo.shape
        f = w1.shape[1]
        assert nh == n and dh * 2 == LANES and r == 256
        cos, sin = _tables(lax.axis_index("seq") * r + jnp.arange(r), dh)
        nm, ngrp, chunk = f // HCOL, n // 4, r + r // 2
        vm = pl.BlockSpec(memory_space=pltpu.VMEM)
        hbm = pl.BlockSpec(memory_space=pl.ANY)
        dma = pltpu.SemaphoreType.DMA
        return pl.pallas_call(
            functools.partial(_kernel, n),
            out_shape=jax.ShapeDtypeStruct((r, d), BF16),
            in_specs=[vm] * 7 + [hbm] * 4,
            out_specs=vm,
            scratch_shapes=[
                pltpu.VMEM((ngrp, 3, d, d // ngrp), BF16), pltpu.VMEM((d, d), BF16),
                pltpu.VMEM((nm, d, HCOL), BF16), pltpu.VMEM((nm, HCOL, d), BF16),
                pltpu.VMEM((r, d), BF16), pltpu.VMEM((r, d), BF16), pltpu.VMEM((r, d), F32),
                pltpu.VMEM((n, chunk, LANES), BF16), pltpu.VMEM((n, chunk, LANES), BF16),
                pltpu.VMEM((n, r, r), F32),
                pltpu.VMEM((n, r // 2, LANES), BF16), pltpu.VMEM((n, r // 2, LANES), BF16),
                pltpu.VMEM((r, d), BF16),
                dma((ngrp, 3)), dma, dma((nm,)), dma((nm,)),
                dma((n,)), dma((n,)), dma((n,)), dma((n,)),
            ],
            compiler_params=pltpu.CompilerParams(
                collective_id=0, has_side_effects=True, vmem_limit_bytes=62 * 2 ** 20),
            name="layer",
        )(x, g1[None], b1[None], g2[None], b2[None], cos, sin, wqkv, wo.reshape(nh * dh, d), w1, w2)

    rows = P(("data", "seq"), None)
    rep = P()
    return jax.shard_map(local, mesh=mesh,
                         in_specs=(rows, rep, rep, rep, rep, rep, rep, rep, rep),
                         out_specs=rows, check_vma=False)
```

```python
import functools
import math

import jax
import jax.numpy as jnp
from jax import lax
from jax.experimental import pallas as pl
from jax.experimental.pallas import tpu as pltpu
from jax.sharding import PartitionSpec as P

EPS = 1e-5
NEG = -1e30
F32 = jnp.float32
BF16 = jnp.bfloat16
LANES = 128
HCOL = 512


def _roll(t, shift):
    return pltpu.roll(t, shift, 1)


def _low(shape):
    return lax.broadcasted_iota(jnp.int32, shape, 1) < LANES // 2


def _pair(top, bot):
    low = _low(top.shape)
    return jnp.where(low, top, _roll(bot, LANES // 2)), jnp.where(low, _roll(top, LANES // 2), bot)


def _transposed(t):
    return t.reshape(t.shape[0] // 8, 8, t.shape[1])


def _kernel(n, scale, x_ref, g1_ref, b1_ref, g2_ref, b2_ref, cos_ref, sin_ref, wqkv_ref, wo_ref, w1_ref, w2_ref, y_ref,
            wq_v, wo_v, w1_v, w2_v, a_v, m_v, acc_v, send, recv, qp_v, s_v, top_v, den_v, out_v, o_send, o_recv, o_v,
            wq_sem, wo_sem, w1_sem, w2_sem, send_sem, recv_sem, osend_sem, orecv_sem):
    r, d = x_ref.shape
    dh = LANES // 2
    chips = n // 2
    ngrp = n // 4
    gcol = d // ngrp
    nm = w1_v.shape[0]
    me = lax.axis_index("seq")
    chip, core = me // 2, me % 2
    odd = chip % 2

    barrier = pltpu.get_barrier_semaphore()

    def greet(i, _):
        pl.semaphore_signal(barrier, inc=1, device_id={"seq": (me + i) % n})
        return 0

    lax.fori_loop(1, n, greet, 0)

    def group(s):
        return (chip // 2 + jnp.where(s == 0, 0, jnp.where(s == 1, 1, jnp.where(s == 2, ngrp - 1, 2)))) % ngrp

    def wq_copy(s, t):
        col = pl.multiple_of(t * d + group(s) * gcol, gcol)
        return pltpu.make_async_copy(wqkv_ref.at[:, pl.ds(col, gcol)], wq_v.at[s, t], wq_sem.at[s, t])

    def w1_copy(i):
        return pltpu.make_async_copy(w1_ref.at[:, pl.ds(pl.multiple_of(i * HCOL, HCOL), HCOL)], w1_v.at[i], w1_sem.at[i])

    def w2_copy(i):
        return pltpu.make_async_copy(w2_ref.at[pl.ds(pl.multiple_of(i * HCOL, HCOL), HCOL), :], w2_v.at[i], w2_sem.at[i])

    wo_copy = pltpu.make_async_copy(wo_ref, wo_v, wo_sem)

    for s in range(ngrp):
        for t in range(3):
            wq_copy(s, t).start()

    xf = x_ref[...].astype(F32)
    mu = jnp.mean(xf, axis=-1, keepdims=True)
    xc = xf - mu
    var = jnp.mean(jnp.square(xc), axis=-1, keepdims=True)
    xn = xc * lax.rsqrt(var + EPS)
    a_v[...] = (xn * g1_ref[...] + b1_ref[...]).astype(BF16)
    m_v[...] = (xn * g2_ref[...] + b2_ref[...]).astype(BF16)
    acc_v[...] = xf
    pl.semaphore_wait(barrier, n - 1)

    def rope(t):
        t = t.astype(BF16).astype(F32)
        lane = lax.broadcasted_iota(jnp.int32, t.shape, 1)
        partner = jnp.where(lane % 64 < 32, _roll(t, LANES - 32), _roll(t, 32))
        return t * cos_ref[...] + partner * sin_ref[...]

    def ship(dst, src, land, ssem, rsem):
        @pl.when(dst == me)
        def _():
            pltpu.make_async_copy(src.at[dst], land.at[me], rsem.at[me]).start()

        @pl.when(dst != me)
        def _():
            pltpu.make_async_remote_copy(
                src_ref=src.at[dst], dst_ref=land.at[me], send_sem=ssem.at[dst], recv_sem=rsem.at[me],
                device_id={"seq": dst}).start()

    def qkv_step(s, _):
        g = group(s)
        for t in range(3):
            wq_copy(s, t).wait()
        for i in range(nm // ngrp):
            w1_copy(s * (nm // ngrp) + i).start()
            w2_copy(s * (nm // ngrp) + i).start()
        a = a_v[...]
        q, k, v = (jnp.dot(a, wq_v[s, t], preferred_element_type=F32) for t in range(3))
        vt = v.T.astype(BF16)
        for j in range(2):
            cols = slice(j * LANES, (j + 1) * LANES)
            kq = _pair(rope(k[:, cols]), rope(q[:, cols]))
            for e in range(2):
                h = 2 * j + e
                send[4 * g + h, :r, :] = kq[e].astype(BF16)
                for c in range(r // LANES):
                    send[4 * g + h, r + c * dh:r + (c + 1) * dh, :] = vt[h * dh:(h + 1) * dh, c * LANES:(c + 1) * LANES]
        near = jnp.where(s == 0, odd, jnp.where(s == 1, 0, jnp.where(s == 2, 1, 1 - odd)))
        for i in range(4):
            ship(4 * g + 2 * (near + i // 2 - 2 * near * (i // 2)) + i % 2, send, recv, send_sem, recv_sem)
        return 0

    lax.fori_loop(0, ngrp, qkv_step, 0)
    wo_copy.start()

    def mlp_step(i, _):
        w1_copy(i).wait()
        w2_copy(i).wait()
        u = jnp.dot(m_v[...], w1_v[i], preferred_element_type=F32)
        h = (0.5 * u * (1.0 + lax.erf(u * (0.5 ** 0.5)))).astype(BF16)
        acc_v[...] += jnp.dot(h, w2_v[i], preferred_element_type=F32)
        return 0

    lax.fori_loop(0, nm, mlp_step, 0)

    def order(t):
        return (chip + jnp.where(t % 2 == 1, (t + 1) // 2, chips - t // 2)) % chips

    def place(c):
        away = (c + chips - chip) % chips
        return jnp.where(away == 0, 0, jnp.where(away <= chips // 2, 2 * away - 1, 2 * (chips - away)))

    def ready(i):
        last = place(i)
        for j in range(chips):
            last = jnp.where(j <= i, jnp.maximum(last, place(j)), last)
        return last

    def job(i, j, diag):
        for h in range(2):
            qi = 2 * i + h
            halves = range(h + 1) if diag else range(2)
            top = None
            for g in halves:
                sc = lax.dot_general(recv[2 * j + g, :r, :], qp_v[qi], (((1,), (1,)), ((), ())),
                                     preferred_element_type=F32)
                if diag and g == h:
                    key = lax.broadcasted_iota(jnp.int32, sc.shape, 0)
                    row = lax.broadcasted_iota(jnp.int32, sc.shape, 1)
                    sc = jnp.where(key <= row, sc, NEG)
                s_v[h, g] = sc
                part = jnp.max(_transposed(sc), axis=0)
                top = part if top is None else jnp.maximum(top, part)
            top = jnp.max(top, axis=0, keepdims=True)
            if not diag:
                old = top_v[qi]
                top = jnp.maximum(top, old)
                alpha = jnp.exp2((old - top) * scale)
            top_v[qi] = top
            den, out = None, None
            for g in halves:
                p = jnp.exp2(s_v[h, g] * scale - top * scale)
                part = jnp.sum(_transposed(p), axis=0)
                den = part if den is None else den + part
                vt = jnp.concatenate([recv[2 * j + g, r + c * dh:r + (c + 1) * dh, :] for c in range(r // LANES)], axis=1)
                part = jnp.dot(vt, p.astype(BF16), preferred_element_type=F32)
                out = part if out is None else out + part
            if not diag:
                den = den_v[qi] * alpha + den
                out = out_v[qi] * alpha + out
            den_v[qi] = den
            out_v[qi] = out

    def finish(i):
        for h in range(2):
            qi = 2 * i + h
            o = (out_v[qi] / jnp.sum(den_v[qi], axis=0, keepdims=True)).astype(BF16)
            for c in range(r // LANES):
                o_send[qi, c * dh:(c + 1) * dh, :] = o[:, c * LANES:(c + 1) * LANES]
        for h in range(2):
            ship(2 * i + h, o_send, o_recv, osend_sem, orecv_sem)

    def attend(t, _):
        b = order(t)
        for h in range(2):
            pltpu.make_async_copy(send.at[2 * b + h], recv.at[2 * b + h], recv_sem.at[2 * b + h]).wait()
            kq = recv[2 * b + h, :r, :].astype(F32)
            qp_v[2 * b + h] = jnp.where(_low(kq.shape), _roll(kq, dh), 0.0).astype(BF16)
        job(b, b, True)

        def pairs(u, _):
            c = order(t - 1 - u)
            i = jnp.maximum(b, c)
            job(i, jnp.minimum(b, c), False)

            @pl.when((i != b) & (ready(i) == t))
            def _():
                finish(i)
            return 0

        lax.fori_loop(0, t, pairs, 0)

        @pl.when(ready(b) == t)
        def _():
            finish(b)
        return 0

    lax.fori_loop(0, chips, attend, 0)

    def returned(i, _):
        pltpu.make_async_copy(o_send.at[i], o_recv.at[i], orecv_sem.at[i]).wait()
        return 0

    lax.fori_loop(0, n, returned, 0)
    for c in range(r // LANES):
        ot = o_recv[:, c * dh:(c + 1) * dh, :].reshape(n * dh, LANES)
        o_v[c * LANES:(c + 1) * LANES, :] = ot.T
    wo_copy.wait()
    for c in range(d // 256):
        cols = slice(c * 256, (c + 1) * 256)
        y_ref[:, cols] = (acc_v[:, cols] + jnp.dot(o_v[...], wo_v[:, cols], preferred_element_type=F32)).astype(BF16)

    def drained(i, _):
        @pl.when(i != me)
        def _():
            for buf, land, sem in ((send, recv, send_sem), (o_send, o_recv, osend_sem)):
                pltpu.make_async_copy(buf.at[0], land.at[0], sem.at[i]).wait()
        return 0

    lax.fori_loop(0, n, drained, 0)


def _tables(pos, dh):
    half = dh // 2
    inv = 10000.0 ** (-2.0 * jnp.arange(half, dtype=F32) / dh)
    ang = pos.astype(F32)[:, None] * inv[None, :]
    cos, sin = jnp.cos(ang), jnp.sin(ang)
    return jnp.concatenate([cos] * 4, axis=1), jnp.concatenate([-sin, sin, -sin, sin], axis=1)


def solution(mesh):
    n = mesh.shape["seq"]

    def local(x, g1, b1, g2, b2, wqkv, wo, w1, w2):
        r, d = x.shape
        nh, dh, _ = wo.shape
        f = w1.shape[1]
        assert nh == n and dh * 2 == LANES and r == 256
        cos, sin = _tables(lax.axis_index("seq") * r + jnp.arange(r), dh)
        nm, ngrp, chunk = f // HCOL, n // 4, r + r // 2
        vm = pl.BlockSpec(memory_space=pltpu.VMEM)
        hbm = pl.BlockSpec(memory_space=pl.ANY)
        dma = pltpu.SemaphoreType.DMA
        return pl.pallas_call(
            functools.partial(_kernel, n, dh ** -0.5 * math.log2(math.e)),
            out_shape=jax.ShapeDtypeStruct((r, d), BF16),
            in_specs=[vm] * 7 + [hbm] * 4,
            out_specs=vm,
            scratch_shapes=[
                pltpu.VMEM((ngrp, 3, d, d // ngrp), BF16), pltpu.VMEM((d, d), BF16),
                pltpu.VMEM((nm, d, HCOL), BF16), pltpu.VMEM((nm, HCOL, d), BF16),
                pltpu.VMEM((r, d), BF16), pltpu.VMEM((r, d), BF16), pltpu.VMEM((r, d), F32),
                pltpu.VMEM((n, chunk, LANES), BF16), pltpu.VMEM((n, chunk, LANES), BF16),
                pltpu.VMEM((n, r, LANES), BF16), pltpu.VMEM((2, 2, r, r), F32),
                pltpu.VMEM((n, 1, r), F32), pltpu.VMEM((n, 8, r), F32), pltpu.VMEM((n, dh, r), F32),
                pltpu.VMEM((n, r // 2, LANES), BF16), pltpu.VMEM((n, r // 2, LANES), BF16),
                pltpu.VMEM((r, d), BF16),
                dma((ngrp, 3)), dma, dma((nm,)), dma((nm,)),
                dma((n,)), dma((n,)), dma((n,)), dma((n,)),
            ],
            compiler_params=pltpu.CompilerParams(
                collective_id=0, has_side_effects=True, vmem_limit_bytes=62 * 2 ** 20),
            name="layer",
        )(x, g1[None], b1[None], g2[None], b2[None], cos, sin, wqkv, wo.reshape(nh * dh, d), w1, w2)

    rows = P(("data", "seq"), None)
    rep = P()
    return jax.shard_map(local, mesh=mesh,
                         in_specs=(rows, rep, rep, rep, rep, rep, rep, rep, rep),
                         out_specs=rows, check_vma=False)
```

```python
import functools
import math

import jax
import numpy as np
import jax.numpy as jnp
from jax import lax
from jax.experimental import pallas as pl
from jax.experimental.pallas import tpu as pltpu
from jax.sharding import PartitionSpec as P

EPS = 1e-5
NEG = -1e30
F32 = jnp.float32
BF16 = jnp.bfloat16
LANES = 128
HCOL = 512


def _roll(t, shift):
    return pltpu.roll(t, shift, 1)


def _low(shape):
    return lax.broadcasted_iota(jnp.int32, shape, 1) < LANES // 2


def _pair(top, bot):
    low = _low(top.shape)
    return jnp.where(low, top, _roll(bot, LANES // 2)), jnp.where(low, _roll(top, LANES // 2), bot)


def _transposed(t):
    return t.reshape(t.shape[0] // 8, 8, t.shape[1])


def _kernel(n, scale, x_ref, g1_ref, b1_ref, g2_ref, b2_ref, turn_ref, base_ref, wqkv_ref, wo_ref, w1_ref, w2_ref, y_ref,
            x_v, gb_v, turn_v, base_v, rot_v, y_v, in_sem, y_sem, wq_v, wo_v, w1_v, w2_v, a_v, m_v, acc_v, send, recv, k_v, qt_v, s_v, top_v, den_v, out_v, o_send, o_recv, o_v,
            wq_sem, wo_sem, w1_sem, w2_sem, send_sem, recv_sem, osend_sem, orecv_sem):
    r, d = x_v.shape
    dh = LANES // 2
    half = r // 2
    chips = n // 2
    ngrp = n // 4
    gcol = d // ngrp
    nm = w1_v.shape[0]
    me = lax.axis_index("seq")
    chip, core = me // 2, me % 2
    odd = chip % 2

    barrier = pltpu.get_barrier_semaphore()

    def greet(i, _):
        pl.semaphore_signal(barrier, inc=1, device_id={"seq": (me + i) % n})
        return 0

    lax.fori_loop(1, n, greet, 0)
    small = [(x_ref, x_v), (turn_ref, turn_v), (base_ref, base_v)]
    small += [(ref, gb_v.at[i]) for i, ref in enumerate((g1_ref, b1_ref, g2_ref, b2_ref))]
    small = [pltpu.make_async_copy(src, dst, in_sem.at[i]) for i, (src, dst) in enumerate(small)]
    for copy in small:
        copy.start()

    def group(s):
        return (chip // 2 + jnp.where(s == 0, 0, jnp.where(s == 1, 1, jnp.where(s == 2, ngrp - 1, 2)))) % ngrp

    def wq_copy(s, t):
        col = pl.multiple_of(t * d + group(s) * gcol, gcol)
        return pltpu.make_async_copy(wqkv_ref.at[:, pl.ds(col, gcol)], wq_v.at[s, t], wq_sem.at[s, t])

    def w1_copy(i):
        return pltpu.make_async_copy(w1_ref.at[:, pl.ds(pl.multiple_of(i * HCOL, HCOL), HCOL)], w1_v.at[i], w1_sem.at[i])

    def w2_copy(i):
        return pltpu.make_async_copy(w2_ref.at[pl.ds(pl.multiple_of(i * HCOL, HCOL), HCOL), :], w2_v.at[i], w2_sem.at[i])

    wo_copy = pltpu.make_async_copy(wo_ref, wo_v, wo_sem)

    for s in range(ngrp):
        for t in range(3):
            wq_copy(s, t).start()

    for copy in small:
        copy.wait()
    cb, sb = (base_v[i, pl.ds(me, 1), :] for i in range(2))
    rot_v[0] = cb * turn_v[0] - sb * turn_v[1]
    rot_v[1] = sb * turn_v[0] + cb * turn_v[1]
    xf = x_v[...].astype(F32)
    mu = jnp.mean(xf, axis=-1, keepdims=True)
    xc = xf - mu
    var = jnp.mean(jnp.square(xc), axis=-1, keepdims=True)
    xn = xc * lax.rsqrt(var + EPS)
    a_v[...] = (xn * gb_v[0] + gb_v[1]).astype(BF16)
    m_v[...] = (xn * gb_v[2] + gb_v[3]).astype(BF16)
    acc_v[...] = xf
    pl.semaphore_wait(barrier, n - 1)

    def rope(t):
        t = t.astype(BF16).astype(F32)
        lane = lax.broadcasted_iota(jnp.int32, t.shape, 1)
        partner = jnp.where(lane % 64 < 32, _roll(t, LANES - 32), _roll(t, 32))
        return t * rot_v[0] + partner * rot_v[1]

    def ship(dst, src, land, ssem, rsem):
        @pl.when(dst == me)
        def _():
            pltpu.make_async_copy(src.at[dst], land.at[me], rsem.at[me]).start()

        @pl.when(dst != me)
        def _():
            pltpu.make_async_remote_copy(
                src_ref=src.at[dst], dst_ref=land.at[me], send_sem=ssem.at[dst], recv_sem=rsem.at[me],
                device_id={"seq": dst}).start()

    def qkv_step(s, _):
        g = group(s)
        for t in range(3):
            wq_copy(s, t).wait()
        for i in range(nm // ngrp):
            w1_copy(s * (nm // ngrp) + i).start()
            w2_copy(s * (nm // ngrp) + i).start()
        a = a_v[...]
        q, k, v = (jnp.dot(a, wq_v[s, t], preferred_element_type=F32) for t in range(3))
        kr = [rope(k[:, j * LANES:(j + 1) * LANES]) for j in range(2)]
        qr = [rope(q[:, j * LANES:(j + 1) * LANES]) for j in range(2)]
        for j in range(2):
            for e, kk in enumerate(_pair(kr[j][:half], kr[j][half:])):
                send[4 * g + 2 * j + e, :half, :] = kk.astype(BF16)
        for at, t in ((half, jnp.concatenate(qr, axis=1)), (r, v)):
            tt = t.T.astype(BF16)
            for h in range(4):
                for c in range(r // LANES):
                    send[4 * g + h, at + c * dh:at + (c + 1) * dh, :] = tt[h * dh:(h + 1) * dh, c * LANES:(c + 1) * LANES]
        near = jnp.where(s == 0, odd, jnp.where(s == 1, 0, jnp.where(s == 2, 1, 1 - odd)))
        for i in range(4):
            ship(4 * g + 2 * (near + i // 2 - 2 * near * (i // 2)) + i % 2, send, recv, send_sem, recv_sem)
        return 0

    lax.fori_loop(0, ngrp, qkv_step, 0)
    qt_v[:, dh:, :] = jnp.zeros((chips, LANES - dh, 2 * r), BF16)
    wo_copy.start()

    def mlp_step(i, _):
        w1_copy(i).wait()
        w2_copy(i).wait()
        u = jnp.dot(m_v[...], w1_v[i], preferred_element_type=F32)
        h = (0.5 * u * (1.0 + lax.erf(u * (0.5 ** 0.5)))).astype(BF16)
        acc_v[...] += jnp.dot(h, w2_v[i], preferred_element_type=F32)
        return 0

    lax.fori_loop(0, nm, mlp_step, 0)

    def order(t):
        return (chip + jnp.where(t % 2 == 1, (t + 1) // 2, chips - t // 2)) % chips

    def place(c):
        away = (c + chips - chip) % chips
        return jnp.where(away == 0, 0, jnp.where(away <= chips // 2, 2 * away - 1, 2 * (chips - away)))

    def ready(i):
        last = place(i)
        for j in range(chips):
            last = jnp.where(j <= i, jnp.maximum(last, place(j)), last)
        return last

    def job(i, j, diag):
        keys = [r * (h + 1) if diag else 2 * r for h in range(2)]
        for h in range(2):
            s_v[h, :keys[h], :] = jnp.dot(k_v[j, :keys[h], :], qt_v[i, :, h * r:(h + 1) * r], preferred_element_type=F32)
        for h in range(2):
            qi = 2 * i + h
            if diag:
                sc = s_v[h, keys[h] - r:keys[h], :]
                key = lax.broadcasted_iota(jnp.int32, sc.shape, 0)
                row = lax.broadcasted_iota(jnp.int32, sc.shape, 1)
                s_v[h, keys[h] - r:keys[h], :] = jnp.where(key <= row, sc, NEG)
            top = jnp.max(jnp.max(_transposed(s_v[h, :keys[h], :]), axis=0), axis=0, keepdims=True)
            if not diag:
                old = top_v[qi]
                top = jnp.maximum(top, old)
                alpha = jnp.exp2((old - top) * scale)
            top_v[qi] = top
            p = jnp.exp2(s_v[h, :keys[h], :] * scale - top * scale)
            den = jnp.sum(_transposed(p), axis=0)
            vt = jnp.concatenate([recv[2 * j + m // 2, r + (m % 2) * dh:r + (m % 2 + 1) * dh, :]
                                  for m in range(keys[h] // LANES)], axis=1)
            out = jnp.dot(vt, p.astype(BF16), preferred_element_type=F32)
            if not diag:
                den = den_v[qi] * alpha + den
                out = out_v[qi] * alpha + out
            den_v[qi] = den
            out_v[qi] = out

    def finish(i):
        for h in range(2):
            qi = 2 * i + h
            o = (out_v[qi] / jnp.sum(den_v[qi], axis=0, keepdims=True)).astype(BF16)
            for c in range(r // LANES):
                o_send[qi, c * dh:(c + 1) * dh, :] = o[:, c * LANES:(c + 1) * LANES]
        for h in range(2):
            ship(2 * i + h, o_send, o_recv, osend_sem, orecv_sem)

    def attend(t, _):
        b = order(t)
        for h in range(2):
            pltpu.make_async_copy(send.at[2 * b + h], recv.at[2 * b + h], recv_sem.at[2 * b + h]).wait()
            k_v[b, h * r:h * r + half, :] = recv[2 * b + h, :half, :]
            k_v[b, h * r + half:(h + 1) * r, :] = _roll(recv[2 * b + h, :half, :].astype(F32), dh).astype(BF16)
            for c in range(r // LANES):
                qt_v[b, :dh, h * r + c * LANES:h * r + (c + 1) * LANES] = recv[2 * b + h, half + c * dh:half + (c + 1) * dh, :]
        job(b, b, True)

        def before(u, _):
            c = order(u)

            @pl.when(c < b)
            def _():
                job(b, c, False)
            return 0

        lax.fori_loop(0, t, before, 0)

        @pl.when(ready(b) == t)
        def _():
            finish(b)

        def after(u, _):
            c = order(t - 1 - u)

            @pl.when(c > b)
            def _():
                job(c, b, False)

            @pl.when((c > b) & (ready(c) == t))
            def _():
                finish(c)
            return 0

        lax.fori_loop(0, t, after, 0)
        return 0

    lax.fori_loop(0, chips, attend, 0)

    def returned(i, _):
        pltpu.make_async_copy(o_send.at[i], o_recv.at[i], orecv_sem.at[i]).wait()
        return 0

    lax.fori_loop(0, n, returned, 0)
    for c in range(r // LANES):
        ot = o_recv[:, c * dh:(c + 1) * dh, :].reshape(n * dh, LANES)
        o_v[c * LANES:(c + 1) * LANES, :] = ot.T
    wo_copy.wait()
    for c in range(d // 256):
        cols = slice(c * 256, (c + 1) * 256)
        y_v[:, cols] = (acc_v[:, cols] + jnp.dot(o_v[...], wo_v[:, cols], preferred_element_type=F32)).astype(BF16)
        pltpu.make_async_copy(y_v.at[:, cols], y_ref.at[:, cols], y_sem.at[c]).start()

    def drained(i, _):
        @pl.when(i != me)
        def _():
            for buf, land, sem in ((send, recv, send_sem), (o_send, o_recv, osend_sem)):
                pltpu.make_async_copy(buf.at[0], land.at[0], sem.at[i]).wait()
        return 0

    lax.fori_loop(0, n, drained, 0)
    for c in range(d // 256):
        cols = slice(c * 256, (c + 1) * 256)
        pltpu.make_async_copy(y_v.at[:, cols], y_ref.at[:, cols], y_sem.at[c]).wait()


def _tables(r, n, dh):
    inv = 10000.0 ** (-2.0 * np.arange(dh // 2) / dh)
    sign = np.array([-1.0, 1.0, -1.0, 1.0]).repeat(dh // 2)

    def both(pos):
        ang = np.tile(pos[:, None] * inv[None, :], (1, 4))
        return np.stack([np.cos(ang), np.sin(ang) * sign]).astype(np.float32)

    return both(np.arange(r)), both(np.arange(n) * r)


def solution(mesh):
    n = mesh.shape["seq"]

    def local(x, g1, b1, g2, b2, wqkv, wo, w1, w2):
        r, d = x.shape
        nh, dh, _ = wo.shape
        f = w1.shape[1]
        assert nh == n and dh * 2 == LANES and r == 256
        turn, base = _tables(r, n, dh)
        nm, ngrp, chunk = f // HCOL, n // 4, r + r // 2
        hbm = pl.BlockSpec(memory_space=pl.ANY)
        dma = pltpu.SemaphoreType.DMA
        return pl.pallas_call(
            functools.partial(_kernel, n, dh ** -0.5 * math.log2(math.e)),
            out_shape=jax.ShapeDtypeStruct((r, d), BF16),
            in_specs=[hbm] * 11,
            out_specs=hbm,
            scratch_shapes=[
                pltpu.VMEM((r, d), BF16), pltpu.VMEM((4, 1, d), F32), pltpu.VMEM(turn.shape, F32),
                pltpu.VMEM(base.shape, F32), pltpu.VMEM(turn.shape, F32), pltpu.VMEM((r, d), BF16), dma((7,)), dma((d // 256,)),
                pltpu.VMEM((ngrp, 3, d, d // ngrp), BF16), pltpu.VMEM((d, d), BF16),
                pltpu.VMEM((nm, d, HCOL), BF16), pltpu.VMEM((nm, HCOL, d), BF16),
                pltpu.VMEM((r, d), BF16), pltpu.VMEM((r, d), BF16), pltpu.VMEM((r, d), F32),
                pltpu.VMEM((n, chunk, LANES), BF16), pltpu.VMEM((n, chunk, LANES), BF16),
                pltpu.VMEM((n // 2, 2 * r, LANES), BF16), pltpu.VMEM((n // 2, LANES, 2 * r), BF16),
                pltpu.VMEM((2, 2 * r, r), F32),
                pltpu.VMEM((n, 1, r), F32), pltpu.VMEM((n, 8, r), F32), pltpu.VMEM((n, dh, r), F32),
                pltpu.VMEM((n, r // 2, LANES), BF16), pltpu.VMEM((n, r // 2, LANES), BF16),
                pltpu.VMEM((r, d), BF16),
                dma((ngrp, 3)), dma, dma((nm,)), dma((nm,)),
                dma((n,)), dma((n,)), dma((n,)), dma((n,)),
            ],
            compiler_params=pltpu.CompilerParams(
                collective_id=0, has_side_effects=True, vmem_limit_bytes=62 * 2 ** 20),
            name="layer",
        )(x, g1[None], b1[None], g2[None], b2[None], turn, base, wqkv, wo.reshape(nh * dh, d), w1, w2)

    rows = P(("data", "seq"), None)
    rep = P()
    return jax.shard_map(local, mesh=mesh,
                         in_specs=(rows, rep, rep, rep, rep, rep, rep, rep, rep),
                         out_specs=rows, check_vma=False)
```

```python
import functools
import math

import jax
import numpy as np
import jax.numpy as jnp
from jax import lax
from jax.experimental import pallas as pl
from jax.experimental.pallas import tpu as pltpu
from jax.sharding import PartitionSpec as P

EPS = 1e-5
NEG = -1e30
F32 = jnp.float32
BF16 = jnp.bfloat16
LANES = 128
HCOL = 512


def _roll(t, shift):
    return pltpu.roll(t, shift, 1)


def _low(shape):
    return lax.broadcasted_iota(jnp.int32, shape, 1) < LANES // 2


def _pair(top, bot):
    low = _low(top.shape)
    return jnp.where(low, top, _roll(bot, LANES // 2)), jnp.where(low, _roll(top, LANES // 2), bot)


def _transposed(t):
    return t.reshape(t.shape[0] // 8, 8, t.shape[1])


def _kernel(n, scale, x_ref, g1_ref, b1_ref, g2_ref, b2_ref, turn_ref, base_ref, wqkv_ref, wo_ref, w1_ref, w2_ref, y_ref,
            x_v, gb_v, turn_v, base_v, rot_v, y_v, in_sem, y_sem, wq_v, wo_v, w1_v, w2_v, a_v, m_v, acc_v, send, recv, k_v, qt_v, s0_v, s1_v, peak0_v, peak1_v, top_v, den_v, out_v, o_send, o_recv, o_v,
            wq_sem, wo_sem, w1_sem, w2_sem, send_sem, recv_sem, osend_sem, orecv_sem):
    r, d = x_v.shape
    dh = LANES // 2
    half = r // 2
    slots = ((s0_v, peak0_v), (s1_v, peak1_v))
    chips = n // 2
    ngrp = n // 4
    gcol = d // ngrp
    nm = w1_v.shape[0]
    me = lax.axis_index("seq")
    chip, core = me // 2, me % 2
    odd = chip % 2

    barrier = pltpu.get_barrier_semaphore()

    def greet(i, _):
        pl.semaphore_signal(barrier, inc=1, device_id={"seq": (me + i) % n})
        return 0

    lax.fori_loop(1, n, greet, 0)
    small = [(x_ref, x_v), (turn_ref, turn_v), (base_ref, base_v)]
    small += [(ref, gb_v.at[i]) for i, ref in enumerate((g1_ref, b1_ref, g2_ref, b2_ref))]
    small = [pltpu.make_async_copy(src, dst, in_sem.at[i]) for i, (src, dst) in enumerate(small)]
    for copy in small:
        copy.start()

    def group(s):
        return (chip // 2 + jnp.where(s == 0, 0, jnp.where(s == 1, 1, jnp.where(s == 2, ngrp - 1, 2)))) % ngrp

    def wq_copy(s, t):
        col = pl.multiple_of(t * d + group(s) * gcol, gcol)
        return pltpu.make_async_copy(wqkv_ref.at[:, pl.ds(col, gcol)], wq_v.at[s, t], wq_sem.at[s, t])

    def w1_copy(i):
        return pltpu.make_async_copy(w1_ref.at[:, pl.ds(pl.multiple_of(i * HCOL, HCOL), HCOL)], w1_v.at[i], w1_sem.at[i])

    def w2_copy(i):
        return pltpu.make_async_copy(w2_ref.at[pl.ds(pl.multiple_of(i * HCOL, HCOL), HCOL), :], w2_v.at[i], w2_sem.at[i])

    wo_copy = pltpu.make_async_copy(wo_ref, wo_v, wo_sem)

    for s in range(ngrp):
        for t in range(3):
            wq_copy(s, t).start()

    for copy in small:
        copy.wait()
    cb, sb = (base_v[i, pl.ds(me, 1), :] for i in range(2))
    rot_v[0] = cb * turn_v[0] - sb * turn_v[1]
    rot_v[1] = sb * turn_v[0] + cb * turn_v[1]
    xf = x_v[...].astype(F32)
    mu = jnp.mean(xf, axis=-1, keepdims=True)
    xc = xf - mu
    var = jnp.mean(jnp.square(xc), axis=-1, keepdims=True)
    xn = xc * lax.rsqrt(var + EPS)
    a_v[...] = (xn * gb_v[0] + gb_v[1]).astype(BF16)
    m_v[...] = (xn * gb_v[2] + gb_v[3]).astype(BF16)
    acc_v[...] = xf
    pl.semaphore_wait(barrier, n - 1)

    def rope(t):
        t = t.astype(BF16).astype(F32)
        lane = lax.broadcasted_iota(jnp.int32, t.shape, 1)
        partner = jnp.where(lane % 64 < 32, _roll(t, LANES - 32), _roll(t, 32))
        return t * rot_v[0] + partner * rot_v[1]

    def ship(dst, src, land, ssem, rsem):
        @pl.when(dst == me)
        def _():
            pltpu.make_async_copy(src.at[dst], land.at[me], rsem.at[me]).start()

        @pl.when(dst != me)
        def _():
            pltpu.make_async_remote_copy(
                src_ref=src.at[dst], dst_ref=land.at[me], send_sem=ssem.at[dst], recv_sem=rsem.at[me],
                device_id={"seq": dst}).start()

    def qkv_step(s, _):
        g = group(s)
        for t in range(3):
            wq_copy(s, t).wait()
        for i in range(nm // ngrp):
            w1_copy(s * (nm // ngrp) + i).start()
            w2_copy(s * (nm // ngrp) + i).start()
        a = a_v[...]
        q, k, v = (jnp.dot(a, wq_v[s, t], preferred_element_type=F32) for t in range(3))
        kr = [rope(k[:, j * LANES:(j + 1) * LANES]) for j in range(2)]
        qr = [rope(q[:, j * LANES:(j + 1) * LANES]) for j in range(2)]
        for j in range(2):
            for e, kk in enumerate(_pair(kr[j][:half], kr[j][half:])):
                send[4 * g + 2 * j + e, :half, :] = kk.astype(BF16)
        for at, t in ((half, jnp.concatenate(qr, axis=1)), (r, v)):
            tt = t.T.astype(BF16)
            for h in range(4):
                for c in range(r // LANES):
                    send[4 * g + h, at + c * dh:at + (c + 1) * dh, :] = tt[h * dh:(h + 1) * dh, c * LANES:(c + 1) * LANES]
        near = jnp.where(s == 0, odd, jnp.where(s == 1, 0, jnp.where(s == 2, 1, 1 - odd)))
        for i in range(4):
            ship(4 * g + 2 * (near + i // 2 - 2 * near * (i // 2)) + i % 2, send, recv, send_sem, recv_sem)
        return 0

    lax.fori_loop(0, ngrp, qkv_step, 0)
    qt_v[:, dh:, :] = jnp.zeros((chips, LANES - dh, 2 * r), BF16)
    wo_copy.start()

    def mlp_step(i, _):
        w1_copy(i).wait()
        w2_copy(i).wait()
        u = jnp.dot(m_v[...], w1_v[i], preferred_element_type=F32)
        h = (0.5 * u * (1.0 + lax.erf(u * (0.5 ** 0.5)))).astype(BF16)
        acc_v[...] += jnp.dot(h, w2_v[i], preferred_element_type=F32)
        return 0

    lax.fori_loop(0, nm, mlp_step, 0)

    def order(t):
        return (chip + jnp.where(t % 2 == 1, (t + 1) // 2, chips - t // 2)) % chips

    def place(c):
        away = (c + chips - chip) % chips
        return jnp.where(away == 0, 0, jnp.where(away <= chips // 2, 2 * away - 1, 2 * (chips - away)))

    def ready(i):
        last = place(i)
        for j in range(chips):
            last = jnp.where(j <= i, jnp.maximum(last, place(j)), last)
        return last

    def score(i, j, slot):
        s_v, peak_v = slots[slot]
        for h in range(2):
            sc = jnp.dot(k_v[j], qt_v[i, :, h * r:(h + 1) * r], preferred_element_type=F32)
            s_v[h] = sc
            peak_v[h] = jnp.max(_transposed(sc), axis=0)

    def absorb(i, j, slot):
        s_v, peak_v = slots[slot]
        for h in range(2):
            qi = 2 * i + h
            old = top_v[qi]
            top = jnp.maximum(jnp.max(peak_v[h], axis=0, keepdims=True), old)
            alpha = jnp.exp2((old - top) * scale)
            top_v[qi] = top
            p = jnp.exp2(s_v[h] * scale - top * scale)
            den_v[qi] = den_v[qi] * alpha + jnp.sum(_transposed(p), axis=0)
            out_v[qi] = out_v[qi] * alpha + jnp.dot(values(j, 2 * r), p.astype(BF16), preferred_element_type=F32)

    def values(j, nk):
        return jnp.concatenate([recv[2 * j + m // 2, r + (m % 2) * dh:r + (m % 2 + 1) * dh, :]
                                for m in range(nk // LANES)], axis=1)

    def diagonal(i, slot):
        s_v, _ = slots[slot]
        for h in range(2):
            qi, nk = 2 * i + h, (h + 1) * r
            s_v[h, :nk, :] = jnp.dot(k_v[i, :nk, :], qt_v[i, :, h * r:(h + 1) * r], preferred_element_type=F32)
            sc = s_v[h, nk - r:nk, :]
            key = lax.broadcasted_iota(jnp.int32, sc.shape, 0)
            row = lax.broadcasted_iota(jnp.int32, sc.shape, 1)
            s_v[h, nk - r:nk, :] = jnp.where(key <= row, sc, NEG)
        for h in range(2):
            qi, nk = 2 * i + h, (h + 1) * r
            top = jnp.max(jnp.max(_transposed(s_v[h, :nk, :]), axis=0), axis=0, keepdims=True)
            top_v[qi] = top
            p = jnp.exp2(s_v[h, :nk, :] * scale - top * scale)
            den_v[qi] = jnp.sum(_transposed(p), axis=0)
            out_v[qi] = jnp.dot(values(i, nk), p.astype(BF16), preferred_element_type=F32)

    def finish(i):
        for h in range(2):
            qi = 2 * i + h
            o = (out_v[qi] / jnp.sum(den_v[qi], axis=0, keepdims=True)).astype(BF16)
            for c in range(r // LANES):
                o_send[qi, c * dh:(c + 1) * dh, :] = o[:, c * LANES:(c + 1) * LANES]
        for h in range(2):
            ship(2 * i + h, o_send, o_recv, osend_sem, orecv_sem)

    def attend(t, _):
        b = order(t)
        for h in range(2):
            pltpu.make_async_copy(send.at[2 * b + h], recv.at[2 * b + h], recv_sem.at[2 * b + h]).wait()
            k_v[b, h * r:h * r + half, :] = recv[2 * b + h, :half, :]
            k_v[b, h * r + half:(h + 1) * r, :] = _roll(recv[2 * b + h, :half, :].astype(F32), dh).astype(BF16)
            for c in range(r // LANES):
                qt_v[b, :dh, h * r + c * LANES:h * r + (c + 1) * LANES] = recv[2 * b + h, half + c * dh:half + (c + 1) * dh, :]
        less = jnp.where(t % 2 == 1, jnp.minimum(b, t), jnp.maximum(b + t + 1 - chips, 0))

        def pick(v):
            v = jnp.maximum(jnp.minimum(v, t - 1), 0)
            return (jnp.where(t % 2 == 1, b + chips - 1 - v, b + t - v)) % chips

        def ahead(v, slot):
            c = pick(v)
            score(jnp.maximum(b, c), jnp.minimum(b, c), slot)

        def take(v, slot):
            c = pick(v)
            absorb(jnp.maximum(b, c), jnp.minimum(b, c), slot)

        def settle(v):
            row = jnp.maximum(b, pick(v))

            @pl.when(((row != b) | (v + 1 == less)) & (ready(row) == t))
            def _():
                finish(row)

        ahead(0, 0)
        diagonal(b, 1)

        @pl.when((less == 0) & (ready(b) == t))
        def _():
            finish(b)

        def pairs(m, _):
            ahead(2 * m + 1, 1)
            take(2 * m, 0)
            settle(2 * m)

            @pl.when(2 * m + 1 < t)
            def _():
                ahead(2 * m + 2, 0)
                take(2 * m + 1, 1)
                settle(2 * m + 1)
            return 0

        lax.fori_loop(0, (t + 1) // 2, pairs, 0)
        return 0

    lax.fori_loop(0, chips, attend, 0)

    def returned(i, _):
        pltpu.make_async_copy(o_send.at[i], o_recv.at[i], orecv_sem.at[i]).wait()
        return 0

    lax.fori_loop(0, n, returned, 0)
    for c in range(r // LANES):
        ot = o_recv[:, c * dh:(c + 1) * dh, :].reshape(n * dh, LANES)
        o_v[c * LANES:(c + 1) * LANES, :] = ot.T
    wo_copy.wait()
    for c in range(d // 256):
        cols = slice(c * 256, (c + 1) * 256)
        y_v[:, cols] = (acc_v[:, cols] + jnp.dot(o_v[...], wo_v[:, cols], preferred_element_type=F32)).astype(BF16)
        pltpu.make_async_copy(y_v.at[:, cols], y_ref.at[:, cols], y_sem.at[c]).start()

    def drained(i, _):
        @pl.when(i != me)
        def _():
            for buf, land, sem in ((send, recv, send_sem), (o_send, o_recv, osend_sem)):
                pltpu.make_async_copy(buf.at[0], land.at[0], sem.at[i]).wait()
        return 0

    lax.fori_loop(0, n, drained, 0)
    for c in range(d // 256):
        cols = slice(c * 256, (c + 1) * 256)
        pltpu.make_async_copy(y_v.at[:, cols], y_ref.at[:, cols], y_sem.at[c]).wait()


def _tables(r, n, dh):
    inv = 10000.0 ** (-2.0 * np.arange(dh // 2) / dh)
    sign = np.array([-1.0, 1.0, -1.0, 1.0]).repeat(dh // 2)

    def both(pos):
        ang = np.tile(pos[:, None] * inv[None, :], (1, 4))
        return np.stack([np.cos(ang), np.sin(ang) * sign]).astype(np.float32)

    return both(np.arange(r)), both(np.arange(n) * r)


def solution(mesh):
    n = mesh.shape["seq"]

    def local(x, g1, b1, g2, b2, wqkv, wo, w1, w2):
        r, d = x.shape
        nh, dh, _ = wo.shape
        f = w1.shape[1]
        assert nh == n and dh * 2 == LANES and r == 256
        turn, base = _tables(r, n, dh)
        nm, ngrp, chunk = f // HCOL, n // 4, r + r // 2
        hbm = pl.BlockSpec(memory_space=pl.ANY)
        dma = pltpu.SemaphoreType.DMA
        return pl.pallas_call(
            functools.partial(_kernel, n, dh ** -0.5 * math.log2(math.e)),
            out_shape=jax.ShapeDtypeStruct((r, d), BF16),
            in_specs=[hbm] * 11,
            out_specs=hbm,
            scratch_shapes=[
                pltpu.VMEM((r, d), BF16), pltpu.VMEM((4, 1, d), F32), pltpu.VMEM(turn.shape, F32),
                pltpu.VMEM(base.shape, F32), pltpu.VMEM(turn.shape, F32), pltpu.VMEM((r, d), BF16), dma((7,)), dma((d // 256,)),
                pltpu.VMEM((ngrp, 3, d, d // ngrp), BF16), pltpu.VMEM((d, d), BF16),
                pltpu.VMEM((nm, d, HCOL), BF16), pltpu.VMEM((nm, HCOL, d), BF16),
                pltpu.VMEM((r, d), BF16), pltpu.VMEM((r, d), BF16), pltpu.VMEM((r, d), F32),
                pltpu.VMEM((n, chunk, LANES), BF16), pltpu.VMEM((n, chunk, LANES), BF16),
                pltpu.VMEM((n // 2, 2 * r, LANES), BF16), pltpu.VMEM((n // 2, LANES, 2 * r), BF16),
                pltpu.VMEM((2, 2 * r, r), F32), pltpu.VMEM((2, 2 * r, r), F32),
                pltpu.VMEM((2, 8, r), F32), pltpu.VMEM((2, 8, r), F32),
                pltpu.VMEM((n, 1, r), F32), pltpu.VMEM((n, 8, r), F32), pltpu.VMEM((n, dh, r), F32),
                pltpu.VMEM((n, r // 2, LANES), BF16), pltpu.VMEM((n, r // 2, LANES), BF16),
                pltpu.VMEM((r, d), BF16),
                dma((ngrp, 3)), dma, dma((nm,)), dma((nm,)),
                dma((n,)), dma((n,)), dma((n,)), dma((n,)),
            ],
            compiler_params=pltpu.CompilerParams(
                collective_id=0, has_side_effects=True, vmem_limit_bytes=62 * 2 ** 20),
            name="layer",
        )(x, g1[None], b1[None], g2[None], b2[None], turn, base, wqkv, wo.reshape(nh * dh, d), w1, w2)

    rows = P(("data", "seq"), None)
    rep = P()
    return jax.shard_map(local, mesh=mesh,
                         in_specs=(rows, rep, rep, rep, rep, rep, rep, rep, rep),
                         out_specs=rows, check_vma=False)
```

```python
import functools
import math

import jax
import numpy as np
import jax.numpy as jnp
from jax import lax
from jax.experimental import pallas as pl
from jax.experimental.pallas import tpu as pltpu
from jax.sharding import PartitionSpec as P

EPS = 1e-5
NEG = -1e30
F32 = jnp.float32
BF16 = jnp.bfloat16
LANES = 128
HCOL = 512


def _roll(t, shift):
    return pltpu.roll(t, shift, 1)


def _low(shape):
    return lax.broadcasted_iota(jnp.int32, shape, 1) < LANES // 2


def _pair(top, bot):
    low = _low(top.shape)
    return jnp.where(low, top, _roll(bot, LANES // 2)), jnp.where(low, _roll(top, LANES // 2), bot)


def _transposed(t):
    return t.reshape(t.shape[0] // 8, 8, t.shape[1])


def _kernel(n, scale, x_ref, g1_ref, b1_ref, g2_ref, b2_ref, turn_ref, base_ref, wqkv_ref, wo_ref, w1_ref, w2_ref, y_ref,
            x_v, gb_v, turn_v, base_v, rot_v, y_v, in_sem, y_sem, wq_v, wo_v, w1_v, w2_v, a_v, m_v, acc_v, send, recv, k_v, qt_v, s0_v, s1_v, peak0_v, peak1_v, top_v, den_v, out_v, o_send, o_recv, o_v,
            wq_sem, wo_sem, w1_sem, w2_sem, send_sem, recv_sem, osend_sem, orecv_sem):
    r, d = x_v.shape
    dh = LANES // 2
    half = r // 2
    slots = ((s0_v, peak0_v), (s1_v, peak1_v))
    chips = n // 2
    ngrp = n // 4
    gcol = d // ngrp
    nm = w1_v.shape[0]
    me = lax.axis_index("seq")
    chip, core = me // 2, me % 2
    odd = chip % 2

    barrier = pltpu.get_barrier_semaphore()

    def greet(i, _):
        pl.semaphore_signal(barrier, inc=1, device_id={"seq": (me + i) % n})
        return 0

    lax.fori_loop(1, n, greet, 0)
    small = [(x_ref, x_v), (turn_ref, turn_v), (base_ref, base_v)]
    small += [(ref, gb_v.at[i]) for i, ref in enumerate((g1_ref, b1_ref, g2_ref, b2_ref))]
    small = [pltpu.make_async_copy(src, dst, in_sem.at[i]) for i, (src, dst) in enumerate(small)]
    for copy in small:
        copy.start()

    def group(s):
        return (chip // 2 + jnp.where(s == 0, 0, jnp.where(s == 1, 1, jnp.where(s == 2, ngrp - 1, 2)))) % ngrp

    def wq_copy(s, t):
        col = pl.multiple_of(t * d + group(s) * gcol, gcol)
        return pltpu.make_async_copy(wqkv_ref.at[:, pl.ds(col, gcol)], wq_v.at[s, t], wq_sem.at[s, t])

    def w1_copy(i):
        return pltpu.make_async_copy(w1_ref.at[:, pl.ds(pl.multiple_of(i * HCOL, HCOL), HCOL)], w1_v.at[i], w1_sem.at[i])

    def w2_copy(i):
        return pltpu.make_async_copy(w2_ref.at[pl.ds(pl.multiple_of(i * HCOL, HCOL), HCOL), :], w2_v.at[i], w2_sem.at[i])

    wo_copy = pltpu.make_async_copy(wo_ref, wo_v, wo_sem)

    for s in range(2):
        for t in range(3):
            wq_copy(s, t).start()

    for copy in small:
        copy.wait()
    cb, sb = (base_v[i, pl.ds(me, 1), :] for i in range(2))
    rot_v[0] = cb * turn_v[0] - sb * turn_v[1]
    rot_v[1] = sb * turn_v[0] + cb * turn_v[1]
    xf = x_v[...].astype(F32)
    mu = jnp.mean(xf, axis=-1, keepdims=True)
    xc = xf - mu
    var = jnp.mean(jnp.square(xc), axis=-1, keepdims=True)
    xn = xc * lax.rsqrt(var + EPS)
    a_v[...] = (xn * gb_v[0] + gb_v[1]).astype(BF16)
    m_v[...] = (xn * gb_v[2] + gb_v[3]).astype(BF16)
    acc_v[...] = xf

    def rope(t):
        t = t.astype(BF16).astype(F32)
        lane = lax.broadcasted_iota(jnp.int32, t.shape, 1)
        partner = jnp.where(lane % 64 < 32, _roll(t, LANES - 32), _roll(t, 32))
        return t * rot_v[0] + partner * rot_v[1]

    def ship(dst, src, land, ssem, rsem):
        @pl.when(dst == me)
        def _():
            pltpu.make_async_copy(src.at[dst], land.at[me], rsem.at[me]).start()

        @pl.when(dst != me)
        def _():
            pltpu.make_async_remote_copy(
                src_ref=src.at[dst], dst_ref=land.at[me], send_sem=ssem.at[dst], recv_sem=rsem.at[me],
                device_id={"seq": dst}).start()

    def qkv_step(s, _):
        g = group(s)
        for t in range(3):
            wq_copy(s, t).wait()

        @pl.when(s + 2 < ngrp)
        def _():
            for t in range(3):
                wq_copy(s + 2, t).start()

        for i in range(nm // ngrp):
            w1_copy(s * (nm // ngrp) + i).start()
            w2_copy(s * (nm // ngrp) + i).start()
        a = a_v[...]
        q, k, v = (jnp.dot(a, wq_v[s, t], preferred_element_type=F32) for t in range(3))
        kr = [rope(k[:, j * LANES:(j + 1) * LANES]) for j in range(2)]
        qr = [rope(q[:, j * LANES:(j + 1) * LANES]) for j in range(2)]
        for j in range(2):
            for e, kk in enumerate(_pair(kr[j][:half], kr[j][half:])):
                send[4 * g + 2 * j + e, :half, :] = kk.astype(BF16)
        for at, t in ((half, jnp.concatenate(qr, axis=1)), (r, v)):
            tt = t.T.astype(BF16)
            for h in range(4):
                for c in range(r // LANES):
                    send[4 * g + h, at + c * dh:at + (c + 1) * dh, :] = tt[h * dh:(h + 1) * dh, c * LANES:(c + 1) * LANES]
        @pl.when(s == 0)
        def _():
            pl.semaphore_wait(barrier, n - 1)
        near = jnp.where(s == 0, odd, jnp.where(s == 1, 0, jnp.where(s == 2, 1, 1 - odd)))
        for i in range(4):
            ship(4 * g + 2 * (near + i // 2 - 2 * near * (i // 2)) + i % 2, send, recv, send_sem, recv_sem)
        return 0

    lax.fori_loop(0, ngrp, qkv_step, 0)
    qt_v[:, dh:, :] = jnp.zeros((chips, LANES - dh, 2 * r), BF16)
    wo_copy.start()

    def mlp_step(i, _):
        w1_copy(i).wait()
        w2_copy(i).wait()
        u = jnp.dot(m_v[...], w1_v[i], preferred_element_type=F32)
        h = (0.5 * u * (1.0 + lax.erf(u * (0.5 ** 0.5)))).astype(BF16)
        acc_v[...] += jnp.dot(h, w2_v[i], preferred_element_type=F32)
        return 0

    lax.fori_loop(0, nm, mlp_step, 0)

    def order(t):
        return (chip + jnp.where(t % 2 == 1, (t + 1) // 2, chips - t // 2)) % chips

    def place(c):
        away = (c + chips - chip) % chips
        return jnp.where(away == 0, 0, jnp.where(away <= chips // 2, 2 * away - 1, 2 * (chips - away)))

    def ready(i):
        last = place(i)
        for j in range(chips):
            last = jnp.where(j <= i, jnp.maximum(last, place(j)), last)
        return last

    def score(i, j, slot):
        s_v, peak_v = slots[slot]
        for h in range(2):
            sc = jnp.dot(k_v[j], qt_v[i, :, h * r:(h + 1) * r], preferred_element_type=F32)
            s_v[h] = sc
            peak_v[h] = jnp.max(_transposed(sc), axis=0)

    def absorb(i, j, slot):
        s_v, peak_v = slots[slot]
        for h in range(2):
            qi = 2 * i + h
            old = top_v[qi]
            top = jnp.maximum(jnp.max(peak_v[h], axis=0, keepdims=True), old)
            alpha = jnp.exp2((old - top) * scale)
            top_v[qi] = top
            p = jnp.exp2(s_v[h] * scale - top * scale)
            den_v[qi] = den_v[qi] * alpha + jnp.sum(_transposed(p), axis=0)
            out_v[qi] = out_v[qi] * alpha + jnp.dot(values(j, 2 * r), p.astype(BF16), preferred_element_type=F32)

    def values(j, nk):
        return jnp.concatenate([recv[2 * j + m // 2, r + (m % 2) * dh:r + (m % 2 + 1) * dh, :]
                                for m in range(nk // LANES)], axis=1)

    def diagonal(i, slot):
        s_v, _ = slots[slot]
        for h in range(2):
            qi, nk = 2 * i + h, (h + 1) * r
            s_v[h, :nk, :] = jnp.dot(k_v[i, :nk, :], qt_v[i, :, h * r:(h + 1) * r], preferred_element_type=F32)
            sc = s_v[h, nk - r:nk, :]
            key = lax.broadcasted_iota(jnp.int32, sc.shape, 0)
            row = lax.broadcasted_iota(jnp.int32, sc.shape, 1)
            s_v[h, nk - r:nk, :] = jnp.where(key <= row, sc, NEG)
        for h in range(2):
            qi, nk = 2 * i + h, (h + 1) * r
            top = jnp.max(jnp.max(_transposed(s_v[h, :nk, :]), axis=0), axis=0, keepdims=True)
            top_v[qi] = top
            p = jnp.exp2(s_v[h, :nk, :] * scale - top * scale)
            den_v[qi] = jnp.sum(_transposed(p), axis=0)
            out_v[qi] = jnp.dot(values(i, nk), p.astype(BF16), preferred_element_type=F32)

    def finish(i):
        for h in range(2):
            qi = 2 * i + h
            o = (out_v[qi] / jnp.sum(den_v[qi], axis=0, keepdims=True)).astype(BF16)
            for c in range(r // LANES):
                o_send[qi, c * dh:(c + 1) * dh, :] = o[:, c * LANES:(c + 1) * LANES]
        for h in range(2):
            ship(2 * i + h, o_send, o_recv, osend_sem, orecv_sem)

    def attend(t, _):
        b = order(t)
        for h in range(2):
            pltpu.make_async_copy(send.at[2 * b + h], recv.at[2 * b + h], recv_sem.at[2 * b + h]).wait()
            k_v[b, h * r:h * r + half, :] = recv[2 * b + h, :half, :]
            k_v[b, h * r + half:(h + 1) * r, :] = _roll(recv[2 * b + h, :half, :].astype(F32), dh).astype(BF16)
            for c in range(r // LANES):
                qt_v[b, :dh, h * r + c * LANES:h * r + (c + 1) * LANES] = recv[2 * b + h, half + c * dh:half + (c + 1) * dh, :]
        less = jnp.where(t % 2 == 1, jnp.minimum(b, t), jnp.maximum(b + t + 1 - chips, 0))

        def pick(v):
            v = jnp.maximum(jnp.minimum(v, t - 1), 0)
            return (jnp.where(t % 2 == 1, b + chips - 1 - v, b + t - v)) % chips

        def ahead(v, slot):
            c = pick(v)
            score(jnp.maximum(b, c), jnp.minimum(b, c), slot)

        def take(v, slot):
            c = pick(v)
            absorb(jnp.maximum(b, c), jnp.minimum(b, c), slot)

        def settle(v):
            row = jnp.maximum(b, pick(v))

            @pl.when(((row != b) | (v + 1 == less)) & (ready(row) == t))
            def _():
                finish(row)

        ahead(0, 0)
        diagonal(b, 1)

        @pl.when((less == 0) & (ready(b) == t))
        def _():
            finish(b)

        def pairs(m, _):
            ahead(2 * m + 1, 1)
            take(2 * m, 0)
            settle(2 * m)

            @pl.when(2 * m + 1 < t)
            def _():
                ahead(2 * m + 2, 0)
                take(2 * m + 1, 1)
                settle(2 * m + 1)
            return 0

        lax.fori_loop(0, (t + 1) // 2, pairs, 0)
        return 0

    lax.fori_loop(0, chips, attend, 0)

    def returned(i, _):
        pltpu.make_async_copy(o_send.at[i], o_recv.at[i], orecv_sem.at[i]).wait()
        return 0

    lax.fori_loop(0, n, returned, 0)
    for c in range(r // LANES):
        ot = o_recv[:, c * dh:(c + 1) * dh, :].reshape(n * dh, LANES)
        o_v[c * LANES:(c + 1) * LANES, :] = ot.T
    wo_copy.wait()
    for c in range(d // 256):
        cols = slice(c * 256, (c + 1) * 256)
        y_v[:, cols] = (acc_v[:, cols] + jnp.dot(o_v[...], wo_v[:, cols], preferred_element_type=F32)).astype(BF16)
        pltpu.make_async_copy(y_v.at[:, cols], y_ref.at[:, cols], y_sem.at[c]).start()

    def drained(i, _):
        @pl.when(i != me)
        def _():
            for buf, land, sem in ((send, recv, send_sem), (o_send, o_recv, osend_sem)):
                pltpu.make_async_copy(buf.at[0], land.at[0], sem.at[i]).wait()
        return 0

    lax.fori_loop(0, n, drained, 0)
    for c in range(d // 256):
        cols = slice(c * 256, (c + 1) * 256)
        pltpu.make_async_copy(y_v.at[:, cols], y_ref.at[:, cols], y_sem.at[c]).wait()


def _tables(r, n, dh):
    inv = 10000.0 ** (-2.0 * np.arange(dh // 2) / dh)
    sign = np.array([-1.0, 1.0, -1.0, 1.0]).repeat(dh // 2)

    def both(pos):
        ang = np.tile(pos[:, None] * inv[None, :], (1, 4))
        return np.stack([np.cos(ang), np.sin(ang) * sign]).astype(np.float32)

    return both(np.arange(r)), both(np.arange(n) * r)


def solution(mesh):
    n = mesh.shape["seq"]

    def local(x, g1, b1, g2, b2, wqkv, wo, w1, w2):
        r, d = x.shape
        nh, dh, _ = wo.shape
        f = w1.shape[1]
        assert nh == n and dh * 2 == LANES and r == 256
        turn, base = _tables(r, n, dh)
        nm, ngrp, chunk = f // HCOL, n // 4, r + r // 2
        hbm = pl.BlockSpec(memory_space=pl.ANY)
        dma = pltpu.SemaphoreType.DMA
        return pl.pallas_call(
            functools.partial(_kernel, n, dh ** -0.5 * math.log2(math.e)),
            out_shape=jax.ShapeDtypeStruct((r, d), BF16),
            in_specs=[hbm] * 11,
            out_specs=hbm,
            scratch_shapes=[
                pltpu.VMEM((r, d), BF16), pltpu.VMEM((4, 1, d), F32), pltpu.VMEM(turn.shape, F32),
                pltpu.VMEM(base.shape, F32), pltpu.VMEM(turn.shape, F32), pltpu.VMEM((r, d), BF16), dma((7,)), dma((d // 256,)),
                pltpu.VMEM((ngrp, 3, d, d // ngrp), BF16), pltpu.VMEM((d, d), BF16),
                pltpu.VMEM((nm, d, HCOL), BF16), pltpu.VMEM((nm, HCOL, d), BF16),
                pltpu.VMEM((r, d), BF16), pltpu.VMEM((r, d), BF16), pltpu.VMEM((r, d), F32),
                pltpu.VMEM((n, chunk, LANES), BF16), pltpu.VMEM((n, chunk, LANES), BF16),
                pltpu.VMEM((n // 2, 2 * r, LANES), BF16), pltpu.VMEM((n // 2, LANES, 2 * r), BF16),
                pltpu.VMEM((2, 2 * r, r), F32), pltpu.VMEM((2, 2 * r, r), F32),
                pltpu.VMEM((2, 8, r), F32), pltpu.VMEM((2, 8, r), F32),
                pltpu.VMEM((n, 1, r), F32), pltpu.VMEM((n, 8, r), F32), pltpu.VMEM((n, dh, r), F32),
                pltpu.VMEM((n, r // 2, LANES), BF16), pltpu.VMEM((n, r // 2, LANES), BF16),
                pltpu.VMEM((r, d), BF16),
                dma((ngrp, 3)), dma, dma((nm,)), dma((nm,)),
                dma((n,)), dma((n,)), dma((n,)), dma((n,)),
            ],
            compiler_params=pltpu.CompilerParams(
                collective_id=0, has_side_effects=True, vmem_limit_bytes=62 * 2 ** 20),
            name="layer",
        )(x, g1[None], b1[None], g2[None], b2[None], turn, base, wqkv, wo.reshape(nh * dh, d), w1, w2)

    rows = P(("data", "seq"), None)
    rep = P()
    return jax.shard_map(local, mesh=mesh,
                         in_specs=(rows, rep, rep, rep, rep, rep, rep, rep, rep),
                         out_specs=rows, check_vma=False)
```
